32 devices in a mesh: dep: 4 (over z), col: 2 (over y), row: 4 (over x, core).
Axes of the slice: x: 2, y: 2, z: 4, core: 2. Of those that a mesh axis runs over, the one named last changes fastest.
Arguments:
- tokens: bfloat16 [32768, 1280], P(('dep', 'row'), 'col')
- w_up1: bfloat16 [1280, 5120], P('row', 'col')
- w_down1: bfloat16 [5120, 1280], P('row', 'col')
- w_up2: bfloat16 [1280, 5120], P('row', 'col')
- w_down2: bfloat16 [5120, 1280], P('row', 'col')
- grad_out: bfloat16 [32768, 1280], P(('dep', 'row'), 'col')
Outputs:
- output 1: bfloat16 [32768, 1280], P(('dep', 'row'), 'col')
- output 2: bfloat16 [32768, 1280], P(('dep', 'row'), 'col')
- output 3: float32 [1280, 5120], P('row', 'col')
- output 4: float32 [5120, 1280], P('row', 'col')
- output 5: float32 [1280, 5120], P('row', 'col')
- output 6: float32 [5120, 1280], P('row', 'col')
All inputs are finite; a program needn't handle non-finite values.
Results may differ from the reference program's by a relative error of at most 0.00457.
Values are sent between devices in bfloat16 or wider.
A program may use at most 1 GiB of HBM per device.

```python
import math
import jax
import jax.numpy as jnp
from jax import lax

HIDDEN = 1280
FFN_DIM = 5120
TOKENS = 32768
ROW_BLOCK = math.gcd(TOKENS, 512)
NUM_BLOCKS = TOKENS // ROW_BLOCK


def setup_inputs(seed: int = 0) -> dict:
    keys = jax.random.split(jax.random.key(seed), 6)
    tokens = jax.random.normal(keys[0], (TOKENS, HIDDEN), jnp.float32)
    w_up1 = jax.random.normal(keys[1], (HIDDEN, FFN_DIM), jnp.float32) * HIDDEN ** -0.5
    w_down1 = jax.random.normal(keys[2], (FFN_DIM, HIDDEN), jnp.float32) * FFN_DIM ** -0.5
    w_up2 = jax.random.normal(keys[3], (HIDDEN, FFN_DIM), jnp.float32) * HIDDEN ** -0.5
    w_down2 = jax.random.normal(keys[4], (FFN_DIM, HIDDEN), jnp.float32) * FFN_DIM ** -0.5
    grad_out = jax.random.normal(keys[5], (TOKENS, HIDDEN), jnp.float32)
    return {
        "tokens": tokens.astype(jnp.bfloat16),
        "w_up1": w_up1.astype(jnp.bfloat16),
        "w_down1": w_down1.astype(jnp.bfloat16),
        "w_up2": w_up2.astype(jnp.bfloat16),
        "w_down2": w_down2.astype(jnp.bfloat16),
        "grad_out": grad_out.astype(jnp.bfloat16),
    }


def gelu_tanh(pre_act):
    return jax.nn.gelu(pre_act, approximate=True)


def gelu_grad(pre_act, grad_hidden):
    return jax.vjp(gelu_tanh, pre_act)[1](grad_hidden)[0]


def dot_last(left_op, right_op):
    return lax.dot_general(left_op, right_op, (((1,), (1,)), ((), ())), preferred_element_type=jnp.float32)


def dot_first(left_op, right_op):
    return lax.dot_general(left_op, right_op, (((0,), (0,)), ((), ())), preferred_element_type=jnp.float32)


def block_forward(block_in, w_up, w_down):
    pre_act = jnp.dot(block_in, w_up, preferred_element_type=jnp.float32)
    hidden = gelu_tanh(pre_act).astype(jnp.bfloat16)
    mlp_out = jnp.dot(hidden, w_down, preferred_element_type=jnp.float32)
    result = (block_in.astype(jnp.float32) + mlp_out).astype(jnp.bfloat16)
    return result, pre_act, hidden


def block_backward(block_in, pre_act, hidden, w_up, w_down, grad_res):
    grad_hidden = dot_last(grad_res, w_down)
    grad_pre = gelu_grad(pre_act, grad_hidden).astype(jnp.bfloat16)
    grad_in = (grad_res.astype(jnp.float32) + dot_last(grad_pre, w_up)).astype(jnp.bfloat16)
    grad_up = dot_first(block_in, grad_pre)
    grad_down = dot_first(hidden, grad_res)
    return grad_in, grad_up, grad_down


def reference(tokens, w_up1, w_down1, w_up2, w_down2, grad_out):
    def scan_step(grad_sums, inputs):
        tok_blk, grad_blk = inputs
        mid_acts, pre_first, hidden_first = block_forward(tok_blk, w_up1, w_down1)
        y_blk, pre_second, hidden_second = block_forward(mid_acts, w_up2, w_down2)
        grad_mid, grad_up2, grad_down2 = block_backward(mid_acts, pre_second, hidden_second, w_up2, w_down2, grad_blk)
        grad_in, grad_up1, grad_down1 = block_backward(tok_blk, pre_first, hidden_first, w_up1, w_down1, grad_mid)
        new_sums = (grad_sums[0] + grad_up1, grad_sums[1] + grad_down1, grad_sums[2] + grad_up2, grad_sums[3] + grad_down2)
        return new_sums, (y_blk, grad_in)

    zeros_up = jnp.zeros((HIDDEN, FFN_DIM), jnp.float32)
    zeros_down = jnp.zeros((FFN_DIM, HIDDEN), jnp.float32)
    tok_blocks = tokens.reshape(NUM_BLOCKS, ROW_BLOCK, HIDDEN)
    grad_blocks = grad_out.reshape(NUM_BLOCKS, ROW_BLOCK, HIDDEN)
    grad_sums, outs = lax.scan(scan_step, (zeros_up, zeros_down, zeros_up, zeros_down), (tok_blocks, grad_blocks))
    y_out = outs[0].reshape(TOKENS, HIDDEN)
    grad_x = outs[1].reshape(TOKENS, HIDDEN)
    return (y_out, grad_x, grad_sums[0], grad_sums[1], grad_sums[2], grad_sums[3])
```

```python
import functools

import jax
import jax.numpy as jnp
from jax import lax
from jax.experimental import pallas as pl
from jax.experimental.pallas import tpu as pltpu
from jax.sharding import PartitionSpec as P

BF = jnp.bfloat16
F32 = jnp.float32
ROOT_2_PI = 0.7978845608028654
ANY = pl.BlockSpec(memory_space=pl.ANY)


class Place:
    def __init__(self):
        self.z = lax.axis_index("dep")
        self.y = lax.axis_index("col")
        row = lax.axis_index("row")
        self.x = row // 2
        self.k = row % 2
        self.half = self.z % 2

    def device(self, z=None, y=None, x=None, k=None):
        z = self.z if z is None else z
        y = self.y if y is None else y
        x = self.x if x is None else x
        k = self.k if k is None else k
        return {"dep": z, "col": y, "row": 2 * x + k}


def remote(src, dst, send_sem, recv_sem, device):
    return pltpu.make_async_remote_copy(
        src_ref=src, dst_ref=dst, send_sem=send_sem, recv_sem=recv_sem,
        device_id=device, device_id_type=pl.DeviceIdType.MESH)


def dot(left, right):
    return lax.dot_general(left, right, (((1,), (0,)), ((), ())), preferred_element_type=F32)


def dot_last(left, right):
    return lax.dot_general(left, right, (((1,), (1,)), ((), ())), preferred_element_type=F32)


def dot_first(left, right):
    return lax.dot_general(left, right, (((0,), (0,)), ((), ())), preferred_element_type=F32)


def gelu_pair(pre_act):
    tanh = jnp.tanh(ROOT_2_PI * (pre_act + 0.044715 * pre_act * pre_act * pre_act))
    half = 0.5 * (1.0 + tanh)
    slope = half + 0.5 * pre_act * (1.0 - tanh * tanh) * ROOT_2_PI * (1.0 + 3 * 0.044715 * pre_act * pre_act)
    return (pre_act * half).astype(BF), slope


PIECES = [(0, 0, 0), (0, 0, 1), (1, 0, 0), (0, 1, 0), (1, 1, 0), (1, 0, 1), (0, 1, 1), (1, 1, 1)]
N_SEM = 16


def gather_kernel(tok, grad, wu1, wd1, wu2, wd2, tok_full, grad_full, up1, down1, up2, down2,
                  stage_up, stage_down, stage_act, send, recv, local):
    here = Place()

    class Weight:
        def __init__(self, index, own, full):
            self.index, self.own, self.full = index, own, full
            self.rows, self.cols = own.shape

        def slot(self, dx, dy, other, twin=0):
            x = here.x if dx == 0 else 1 - here.x
            y = here.y if dy == 0 else 1 - here.y
            k = here.k if twin == 0 else 1 - here.k
            h = here.half if other == 0 else 1 - here.half
            half_rows = self.rows // 2
            start = pl.multiple_of((2 * x + k) * self.rows + h * half_rows, half_rows)
            return self.full.at[pl.ds(start, half_rows), pl.ds(pl.multiple_of(y * self.cols, self.cols), self.cols)]

        def own_half(self, other):
            h = here.half if other == 0 else 1 - here.half
            half_rows = self.rows // 2
            return self.own.at[pl.ds(pl.multiple_of(h * half_rows, half_rows), half_rows), :]

        def source(self, piece):
            return self.own_half(piece[2]) if piece[:2] == (0, 0) else self.slot(*piece)

        def hop(self, sem, piece, way):
            dx, dy, other = piece
            device = {"x": here.device(x=1 - here.x), "y": here.device(y=1 - here.y), "z": here.device(z=here.z + 1 - 2 * here.half),
                      "core": here.device(k=1 - here.k)}[way]
            arrived = {"x": (1 - dx, dy, other), "y": (dx, 1 - dy, other), "z": (dx, dy, 1 - other), "core": piece}[way]
            copy = remote(self.source(piece), self.slot(*piece), send.at[self.index, sem], recv.at[self.index, sem], device)
            copy.start()
            landed = self.slot(*arrived, twin=1 if way == "core" else 0)
            arrival = remote(landed, landed, send.at[self.index, sem], recv.at[self.index, sem], device)
            return copy, arrival

    weights = [Weight(i, own, full) for i, (own, full) in enumerate(((wu1, up1), (wd1, down1), (wu2, up2), (wd2, down2)))]
    sent = []
    arriving = {}

    def hop(m, piece, way):
        sem = {"x": 0, "y": 1, "z": 2, "core": 3}[way]
        key = (m, piece, way)
        number = len([1 for other in arriving if other[0] == m])
        copy, arrival = weights[m].hop(number, piece, way)
        sent.append(copy)
        arriving[key] = arrival

    def land(m, piece, way):
        arriving[(m, piece, way)].wait_recv()

    def act_copy(src, full, index):
        cols = src.shape[1]
        mine = full.at[:, pl.ds(pl.multiple_of(here.y * cols, cols), cols)]
        copy = remote(src, mine, send.at[4, index], recv.at[4, index], here.device(y=1 - here.y))
        copy.start()
        sent.append(copy)
        return copy

    def stage_in(src, buf, index):
        pltpu.make_async_copy(src, buf, local.at[index]).start()

    stages = [(wu1, stage_up.at[0], up1), (wd1, stage_down.at[0], down1), (wu2, stage_up.at[1], up2), (wd2, stage_down.at[1], down2)]

    def open_weight(m):
        hop(m, (0, 0, 0), "x")
        hop(m, (0, 0, 0), "y")
        hop(m, (0, 0, 0), "core")
        hop(m, (0, 0, 1), "core")

    def second(m):
        land(m, (0, 0, 0), "y")
        hop(m, (0, 1, 0), "x")
        hop(m, (0, 1, 0), "z")
        hop(m, (0, 1, 0), "core")
        land(m, (0, 0, 0), "x")
        hop(m, (1, 0, 0), "z")
        hop(m, (1, 0, 0), "core")

    def third(m):
        land(m, (0, 1, 0), "x")
        hop(m, (1, 1, 0), "z")
        hop(m, (1, 1, 0), "core")
        land(m, (0, 1, 0), "z")
        hop(m, (0, 1, 1), "core")
        land(m, (1, 0, 0), "z")
        hop(m, (1, 0, 1), "core")

    def fourth(m):
        land(m, (1, 1, 0), "z")
        hop(m, (1, 1, 1), "core")
        for piece in PIECES:
            land(m, piece, "core")

    open_weight(0)
    tok_copy = act_copy(tok, tok_full, 0)
    for i, (src, buf, full) in enumerate(stages):
        stage_in(src, buf, i)
    for i, src in enumerate((tok, grad)):
        stage_in(src, stage_act.at[i], 4 + i)
    outs = []
    for i, (src, buf, full) in enumerate(stages):
        pltpu.make_async_copy(src, buf, local.at[i]).wait()
        rows, cols = src.shape
        place = full.at[pl.ds(pl.multiple_of((2 * here.x + here.k) * rows, rows), rows), pl.ds(pl.multiple_of(here.y * cols, cols), cols)]
        outs.append(pltpu.make_async_copy(buf, place, local.at[i]))
        outs[-1].start()
    for i, (src, full) in enumerate(((tok, tok_full), (grad, grad_full))):
        pltpu.make_async_copy(src, stage_act.at[i], local.at[4 + i]).wait()
        cols = src.shape[1]
        place = full.at[:, pl.ds(pl.multiple_of(here.y * cols, cols), cols)]
        outs.append(pltpu.make_async_copy(stage_act.at[i], place, local.at[4 + i]))
        outs[-1].start()
    for m in range(4):
        second(m)
        if m < 3:
            open_weight(m + 1)
        if m == 2:
            grad_copy = act_copy(grad, grad_full, 1)
        third(m)
        if m > 0:
            fourth(m - 1)
    fourth(3)

    def landed_act(src, full, index):
        cols = src.shape[1]
        other = full.at[:, pl.ds(pl.multiple_of((1 - here.y) * cols, cols), cols)]
        remote(other, other, send.at[4, index], recv.at[4, index], here.device(y=1 - here.y)).wait_recv()

    landed_act(tok, tok_full, 0)
    landed_act(grad, grad_full, 1)
    for copy in sent:
        copy.wait_send()
    for copy in outs:
        copy.wait()


def gather_all(tok, wu1, wd1, wu2, wd2, grad):
    t, h = tok.shape
    r1, c1 = wu1.shape
    r2, c2 = wd1.shape
    shape = jax.ShapeDtypeStruct
    return pl.pallas_call(
        gather_kernel,
        out_shape=(shape((t, 2 * h), BF), shape((t, 2 * h), BF), shape((4 * r1, 2 * c1), BF), shape((4 * r2, 2 * c2), BF),
                   shape((4 * r1, 2 * c1), BF), shape((4 * r2, 2 * c2), BF)),
        in_specs=[ANY] * 6,
        out_specs=(ANY,) * 6,
        scratch_shapes=[pltpu.VMEM((2, r1, c1), BF), pltpu.VMEM((2, r2, c2), BF), pltpu.VMEM((2, t, h), BF),
                        pltpu.SemaphoreType.DMA((5, N_SEM)), pltpu.SemaphoreType.DMA((5, N_SEM)), pltpu.SemaphoreType.DMA((6,))],
        compiler_params=pltpu.CompilerParams(has_side_effects=True, vmem_limit_bytes=40 * 1024 * 1024),
        name="gather_all",
    )(tok, grad, wu1, wd1, wu2, wd2)


CHUNKS = 4


def reduce_kernel(*refs):
    parts, refs = refs[:4], refs[4:]
    outs, refs = refs[:4], refs[4:]
    from_twin, refs = refs[:4], refs[4:]
    to_x, from_x, mid, from_in, tot, from_ex = [refs[4 * i:4 * i + 4] for i in range(6)]
    refs = refs[24:]
    buf_up, buf_down, send, recv, lsem = refs
    here = Place()
    z_end = (here.z == 0) | (here.z == 3)
    inner = jnp.where(here.z == 0, 1, jnp.where(here.z == 3, 2, 3 - here.z))
    outer = jnp.where(here.z < 2, 0, 3)
    n_chunks = 4 * CHUNKS

    def chunk(ref, c, quarter=None):
        rows = ref.shape[0] // 4 if quarter is not None else ref.shape[0]
        step = rows // CHUNKS
        base = c * step if quarter is None else quarter * rows + c * step
        return ref.at[pl.ds(pl.multiple_of(base, step), step), :]

    def add(dst, *srcs):
        buf = buf_up if srcs[0].shape[1] > 1024 else buf_down
        copies = [pltpu.make_async_copy(src, buf.at[i], lsem.at[i]) for i, src in enumerate(srcs)]
        for copy in copies:
            copy.start()
        for copy in copies:
            copy.wait()
        total = buf[0]
        for i in range(1, len(srcs)):
            total = total + buf[i]
        buf[3] = total
        out = pltpu.make_async_copy(buf.at[3], dst, lsem.at[3])
        out.start()
        out.wait()

    def pair(src, dst, sem, i, device):
        return remote(src, dst, send.at[sem, i], recv.at[sem, i], device)

    def core_copy(i, which):
        m, c = divmod(i, CHUNKS)
        x = 1 - here.x if which == 0 else here.x
        rows = parts[m].shape[0] // 4
        src = chunk(parts[m], c, 2 * x + 1 - here.k)
        dst = from_twin[m].at[which, pl.ds(c * (rows // CHUNKS), rows // CHUNKS), :]
        return pair(src, dst, which, i, here.device(k=1 - here.k))

    def x_copy(i):
        m, c = divmod(i, CHUNKS)
        return pair(chunk(to_x[m], c), chunk(from_x[m], c), 2, i, here.device(x=1 - here.x))

    def in_copy(i):
        m, c = divmod(i, CHUNKS)
        return pair(chunk(mid[m], c), chunk(from_in[m], c), 3, i, here.device(z=inner))

    def ex_copy(i):
        m, c = divmod(i, CHUNKS)
        return pair(chunk(tot[m], c), chunk(from_ex[m], c), 4, i, here.device(z=inner))

    def out_copy(i):
        m, c = divmod(i, CHUNKS)
        return pair(chunk(outs[m], c), chunk(outs[m], c), 5, i, here.device(z=outer))

    def stage_core(i):
        core_copy(i, 0).start()
        core_copy(i, 1).start()

    def stage_x(i):
        m, c = divmod(i, CHUNKS)
        core_copy(i, 0).wait_recv()
        rows = parts[m].shape[0] // 4
        twin = from_twin[m].at[0, pl.ds(c * (rows // CHUNKS), rows // CHUNKS), :]
        add(chunk(to_x[m], c), chunk(parts[m], c, 2 * (1 - here.x) + here.k), twin)
        x_copy(i).start()

    def stage_mid(i):
        m, c = divmod(i, CHUNKS)
        core_copy(i, 1).wait_recv()
        x_copy(i).wait_recv()
        rows = parts[m].shape[0] // 4
        twin = from_twin[m].at[1, pl.ds(c * (rows // CHUNKS), rows // CHUNKS), :]
        add(chunk(mid[m], c), chunk(parts[m], c, 2 * here.x + here.k), twin, chunk(from_x[m], c))

        @pl.when(z_end)
        def _():
            in_copy(i).start()

    def stage_in(i):
        m, c = divmod(i, CHUNKS)

        @pl.when(~z_end)
        def _():
            in_copy(i).wait_recv()
            add(chunk(tot[m], c), chunk(mid[m], c), chunk(from_in[m], c))
            ex_copy(i).start()

    def stage_ex(i):
        m, c = divmod(i, CHUNKS)

        @pl.when(~z_end)
        def _():
            ex_copy(i).wait_recv()
            add(chunk(outs[m], c), chunk(tot[m], c), chunk(from_ex[m], c))
            out_copy(i).start()

    def stage_out(i):
        @pl.when(z_end)
        def _():
            out_copy(i).wait_recv()
            in_copy(i).wait_send()

        @pl.when(~z_end)
        def _():
            ex_copy(i).wait_send()
            out_copy(i).wait_send()

        core_copy(i, 0).wait_send()
        core_copy(i, 1).wait_send()
        x_copy(i).wait_send()

    stages = [stage_core, stage_x, stage_mid, stage_in, stage_ex, stage_out]
    for step in range(n_chunks + len(stages) - 1):
        for s, stage in enumerate(stages):
            if 0 <= step - s < n_chunks:
                stage(step - s)


def reduce_grads(parts):
    shape = jax.ShapeDtypeStruct
    quarters = [(p.shape[0] // 4, p.shape[1]) for p in parts]
    scratch_out = [shape((2,) + q, F32) for q in quarters] + [shape(q, F32) for _ in range(6) for q in quarters]
    up = max(quarters, key=lambda q: q[1])
    down = min(quarters, key=lambda q: q[1])
    n = 4 * CHUNKS
    results = pl.pallas_call(
        reduce_kernel,
        out_shape=tuple([shape(q, F32) for q in quarters] + scratch_out),
        in_specs=[ANY] * 4,
        out_specs=(ANY,) * (4 + len(scratch_out)),
        scratch_shapes=[pltpu.VMEM((4, up[0] // CHUNKS, up[1]), F32), pltpu.VMEM((4, down[0] // CHUNKS, down[1]), F32),
                        pltpu.SemaphoreType.DMA((6, n)), pltpu.SemaphoreType.DMA((6, n)), pltpu.SemaphoreType.DMA((4,))],
        compiler_params=pltpu.CompilerParams(has_side_effects=True, vmem_limit_bytes=40 * 1024 * 1024),
        name="reduce_grads",
    )(*parts)
    return results[:4]


def solution(mesh):
    act_spec = P(("dep", "row"), "col")
    weight_spec = P("row", "col")

    def local_step(tokens, w_up1, w_down1, w_up2, w_down2, grad_out):
        y = lax.axis_index("col")

        def my_cols(arr):
            width = arr.shape[1] // 2
            return lax.dynamic_slice(arr, (0, y * width), (arr.shape[0], width))

        def my_rows(arr):
            height = arr.shape[0] // 2
            return lax.dynamic_slice(arr, (y * height, 0), (height, arr.shape[1]))

        x_full, g_full, up1, down1, up2, down2 = gather_all(tokens, w_up1, w_down1, w_up2, w_down2, grad_out)
        hid1, slope1 = gelu_pair(dot(x_full, up1))
        mid = (x_full.astype(F32) + dot(hid1, down1)).astype(BF)
        hid2, slope2 = gelu_pair(dot(mid, up2))
        part_down2 = dot_first(hid2, grad_out)
        y_out = (my_cols(mid).astype(F32) + dot(hid2, my_cols(down2))).astype(BF)
        dpre2 = (dot_last(g_full, down2) * slope2).astype(BF)
        part_up2 = dot_first(mid, my_cols(dpre2))
        dmid = (g_full.astype(F32) + dot_last(dpre2, up2)).astype(BF)
        part_down1 = dot_first(hid1, my_cols(dmid))
        dpre1 = (dot_last(dmid, down1) * slope1).astype(BF)
        part_up1 = dot_first(x_full, my_cols(dpre1))
        grad_x = (my_cols(dmid).astype(F32) + dot_last(dpre1, my_rows(up1))).astype(BF)
        grad_down2, grad_up2, grad_down1, grad_up1 = reduce_grads([part_down2, part_up2, part_down1, part_up1])
        return y_out, grad_x, grad_up1, grad_down1, grad_up2, grad_down2

    return jax.shard_map(local_step, mesh=mesh, in_specs=(act_spec, weight_spec, weight_spec, weight_spec, weight_spec, act_spec), out_specs=(act_spec, act_spec, weight_spec, weight_spec, weight_spec, weight_spec), check_vma=False)
```

```python
import functools

import jax
import jax.numpy as jnp
from jax import lax
from jax.experimental import pallas as pl
from jax.experimental.pallas import tpu as pltpu
from jax.sharding import PartitionSpec as P

BF = jnp.bfloat16
F32 = jnp.float32
ROOT_2_PI = 0.7978845608028654
CUBIC = 0.044715
ANY = pl.BlockSpec(memory_space=pl.ANY)


class Place:
    def __init__(self):
        self.z = lax.axis_index("dep")
        self.y = lax.axis_index("col")
        row = lax.axis_index("row")
        self.x = row // 2
        self.k = row % 2
        self.half = self.z % 2

    def device(self, z=None, y=None, x=None, k=None):
        z = self.z if z is None else z
        y = self.y if y is None else y
        x = self.x if x is None else x
        k = self.k if k is None else k
        return {"dep": z, "col": y, "row": 2 * x + k}


def remote(src, dst, send_sem, recv_sem, device):
    return pltpu.make_async_remote_copy(
        src_ref=src, dst_ref=dst, send_sem=send_sem, recv_sem=recv_sem,
        device_id=device, device_id_type=pl.DeviceIdType.MESH)


def dot(left, right):
    return lax.dot_general(left, right, (((1,), (0,)), ((), ())), preferred_element_type=F32)


def dot_last(left, right):
    return lax.dot_general(left, right, (((1,), (1,)), ((), ())), preferred_element_type=F32)


def dot_first(left, right):
    return lax.dot_general(left, right, (((0,), (0,)), ((), ())), preferred_element_type=F32)


def gelu_pair(pre_act):
    square = pre_act * pre_act
    half = 0.5 + 0.5 * jnp.tanh(pre_act * (ROOT_2_PI + (ROOT_2_PI * CUBIC) * square))
    slope = half + ((half - half * half) * pre_act) * (2 * ROOT_2_PI + (6 * CUBIC * ROOT_2_PI) * square)
    return (pre_act * half).astype(BF), slope


CONTRACT = {"nn": (((1,), (0,)), ((), ())), "nt": (((1,), (1,)), ((), ())), "tn": (((0,), (0,)), ((), ()))}


def matmul(left, right, outs, form, tile, epilogue, extra=(), rows_inner=True, hooks=()):
    depth = left.shape[0] if form == "tn" else left.shape[1]
    rows = left.shape[1] if form == "tn" else left.shape[0]
    cols = right.shape[0] if form == "nt" else right.shape[1]
    tm, tn = tile
    grid = (cols // tn, rows // tm) if rows_inner else (rows // tm, cols // tn)
    assert all(at < grid[0] * grid[1] for at, _ in hooks)

    def spec(shape, index):
        return pl.BlockSpec(shape, (lambda n, m: index(m, n)) if rows_inner else index)

    left_spec = spec((depth, tm), lambda m, n: (0, m)) if form == "tn" else spec((tm, depth), lambda m, n: (m, 0))
    right_spec = spec((tn, depth), lambda m, n: (n, 0)) if form == "nt" else spec((depth, tn), lambda m, n: (0, n))
    tile_spec = spec((tm, tn), lambda m, n: (m, n))

    def body(left_ref, right_ref, *rest):
        step = pl.program_id(0) * grid[1] + pl.program_id(1)
        for at, action in hooks:
            pl.when(step == at)(action)
        product = lax.dot_general(left_ref[...], right_ref[...], CONTRACT[form], preferred_element_type=F32)
        results = epilogue(product, *[ref[...] for ref in rest[:len(extra)]])
        for ref, value in zip(rest[len(extra):], results):
            ref[...] = value

    pltpu.emit_pipeline(body, grid=grid, in_specs=[left_spec, right_spec] + [tile_spec] * len(extra),
                        out_specs=[tile_spec] * len(outs))(left, right, *extra, *outs)


def plain(product):
    return (product,)


def residual(product, base):
    return ((base.astype(F32) + product).astype(BF),)


def halves(ref, y):
    width = ref.shape[1] // 2
    return [ref.at[:, pl.ds(pl.multiple_of(h * width, width), width)] for h in (y, 1 - y)]


def tokens_of(ref, part, parts):
    step = ref.shape[0] // parts
    return ref.at[pl.ds(part * step, step), :]


OWN = (0, 0, 0)
OWN_ALL = (0, 0, 2)
X_NEAR = (1, 0, 0)
X_REST = (1, 0, 1)
X_ALL = (1, 0, 2)
Y_NEAR = (0, 1, 0)
Y_REST = (0, 1, 1)
DIAG_NEAR = (1, 1, 0)
DIAG_REST = (1, 1, 1)
UP1, DOWN1, UP2, DOWN2 = range(4)

N_SEM = 16
ACT_PARTS = 4


def forward_kernel(tok, grad, wu1, wd1, wu2, wd2, tok_full, grad_full, up1, down1, up2, down2,
                   hid1, slope1, mid, hid2, slope2, part_down2,
                   stage_up, stage_down, stage_act, send, recv, act_send, act_recv, local):
    here = Place()

    class Weight:
        def __init__(self, index, own, full):
            self.index, self.own, self.full = index, own, full
            self.rows, self.cols = own.shape

        def slot(self, dx, dy, other, twin=0):
            x = here.x if dx == 0 else 1 - here.x
            y = here.y if dy == 0 else 1 - here.y
            k = here.k if twin == 0 else 1 - here.k
            h = 0 if other == 2 else here.half if other == 0 else 1 - here.half
            height = self.rows if other == 2 else self.rows // 2
            start = pl.multiple_of((2 * x + k) * self.rows + h * height, height)
            return self.full.at[pl.ds(start, height), pl.ds(pl.multiple_of(y * self.cols, self.cols), self.cols)]

        def source(self, piece):
            if piece[:2] != (0, 0):
                return self.slot(*piece)
            if piece[2] == 2:
                return self.own
            h = here.half if piece[2] == 0 else 1 - here.half
            height = self.rows // 2
            return self.own.at[pl.ds(pl.multiple_of(h * height, height), height), :]

    weights = [Weight(i, own, full) for i, (own, full) in enumerate(((wu1, up1), (wd1, down1), (wu2, up2), (wd2, down2)))]
    slots = {}
    landed = set()

    def number(m, piece, way):
        return slots.setdefault((m, piece, way), len([key for key in slots if key[0] == m]))

    def neighbour(way):
        return {"x": here.device(x=1 - here.x), "y": here.device(y=1 - here.y), "z": here.device(z=here.z + 1 - 2 * here.half),
                "core": here.device(k=1 - here.k)}[way]

    def beyond(piece, way):
        dx, dy, other = piece
        return {"x": (1 - dx, dy, other), "y": (dx, 1 - dy, other), "z": (dx, dy, 1 - other if other < 2 else 2), "core": piece}[way]

    def hop(m, piece, way, start=True):
        n = number(m, piece, way)
        copy = remote(weights[m].source(piece), weights[m].slot(*piece), send.at[m, n], recv.at[m, n], neighbour(way))
        if start:
            copy.start()
        else:
            copy.wait_send()

    def land(m, way, piece):
        n = number(m, beyond(piece, way), way)
        landed.add((m, beyond(piece, way), way))
        place = weights[m].slot(*piece, twin=1 if way == "core" else 0)
        remote(place, place, send.at[m, n], recv.at[m, n], neighbour(way)).wait_recv()

    def act_copy(src, full, index, part, wait=None):
        cols, height = src.shape[1], src.shape[0] // ACT_PARTS
        rows = pl.ds(part * height, height)

        def place(y):
            return full.at[rows, pl.ds(pl.multiple_of(y * cols, cols), cols)]

        sems = act_send.at[index, part], act_recv.at[index, part]
        if wait == "recv":
            remote(place(1 - here.y), place(1 - here.y), *sems, neighbour("y")).wait_recv()
            return
        copy = remote(src.at[rows, :], place(here.y), *sems, neighbour("y"))
        if wait == "send":
            copy.wait_send()
        else:
            copy.start()

    def land_all(m):
        for key in [key for key in slots if key[0] == m and key[2] == "core" and key not in landed]:
            land(m, "core", key[1])

    hop(UP1, OWN, "x")
    hop(UP1, OWN, "y")
    hop(UP1, OWN_ALL, "core")
    for part in range(ACT_PARTS):
        if part == ACT_PARTS - 1:
            hop(DOWN1, OWN, "y")
        act_copy(tok, tok_full, 0, part)
    for m in (UP2, DOWN2):
        hop(m, OWN, "y")
    for part in range(ACT_PARTS):
        act_copy(grad, grad_full, 1, part)

    stages = [(wu1, stage_up.at[0], up1), (wd1, stage_down.at[0], down1), (wu2, stage_up.at[1], up2), (wd2, stage_down.at[1], down2)]
    own_places = []
    for src, buf, full in stages:
        rows, cols = src.shape
        own_places.append((src, buf, full.at[pl.ds(pl.multiple_of((2 * here.x + here.k) * rows, rows), rows),
                                             pl.ds(pl.multiple_of(here.y * cols, cols), cols)]))
    for i, (src, full) in enumerate(((tok, tok_full), (grad, grad_full))):
        cols = src.shape[1]
        own_places.append((src, stage_act.at[i], full.at[:, pl.ds(pl.multiple_of(here.y * cols, cols), cols)]))
    for i, (src, buf, place) in enumerate(own_places):
        pltpu.make_async_copy(src, buf, local.at[i]).start()
    outs = []
    for i, (src, buf, place) in enumerate(own_places):
        pltpu.make_async_copy(src, buf, local.at[i]).wait()
        outs.append(pltpu.make_async_copy(buf, place, local.at[i]))
        outs[-1].start()
    for copy in outs:
        copy.wait()

    def pass_on(m, way, piece, *ways):
        def action():
            land(m, way, piece)
            for onward in ways:
                hop(m, piece, onward)
            hop(m, piece, "core")
        return action

    def begin(*sends):
        def action():
            for m, piece, way in sends:
                hop(m, piece, way)
        return action

    def run(*actions):
        for action in actions:
            action()

    def up(act, weight, hid, slope, hooks=()):
        rows = act.shape[0]
        matmul(act, weight, (hid, slope), "nn", (rows, 512 if rows < 2048 else 256), gelu_pair, hooks=hooks)

    up1_h, hid1_h, slope1_h = [halves(ref, here.y) for ref in (up1, hid1, slope1)]
    up2_h, hid2_h, slope2_h = [halves(ref, here.y) for ref in (up2, hid2, slope2)]

    def up_part(h, first, count, hooks=()):
        height = tok.shape[0] // ACT_PARTS
        rows = pl.ds(first * height, count * height)
        up(tok_full.at[rows, :], up1_h[h], hid1_h[h].at[rows, :], slope1_h[h].at[rows, :], hooks)

    def tokens_land(*parts):
        for part in parts:
            act_copy(tok, tok_full, 0, part, "recv")

    def near_core(m):
        for piece in (OWN_ALL, X_NEAR, X_REST):
            land(m, "core", piece)

    run(pass_on(UP1, "x", X_NEAR, "z"), pass_on(UP1, "y", Y_NEAR, "x", "z"),
        begin((DOWN1, OWN, "x"), (DOWN1, OWN_ALL, "core"), (UP2, OWN_ALL, "core"), (DOWN2, OWN_ALL, "core")),
        pass_on(UP1, "z", X_REST), pass_on(UP1, "x", DIAG_NEAR, "z"))
    near_core(UP1)
    tokens_land(0, 1)
    up_part(0, 0, 2, [(3, pass_on(UP1, "z", Y_REST)), (4, pass_on(DOWN1, "x", X_NEAR))])
    tokens_land(2)
    up_part(0, 2, 1)
    run(pass_on(UP1, "z", DIAG_REST))
    land_all(UP1)
    up_part(1, 0, 2, [(3, pass_on(DOWN1, "y", Y_NEAR, "x", "z")), (3, begin((DOWN1, X_NEAR, "z")))])
    up_part(1, 2, 1)
    run(pass_on(DOWN1, "x", DIAG_NEAR), pass_on(DOWN1, "z", Y_REST, "x"), begin((UP2, OWN, "x")))
    tokens_land(3)
    up_part(0, 3, 1)
    up_part(1, 3, 1, [(2, pass_on(UP2, "y", Y_NEAR, "z", "x"))])
    run(pass_on(DOWN1, "z", X_REST), pass_on(DOWN1, "x", DIAG_REST))
    land_all(DOWN1)
    matmul(hid1, down1, (mid,), "nn", (1024, 256), residual, extra=(tok_full,), rows_inner=False,
           hooks=[(3, pass_on(UP2, "z", Y_REST, "x")), (5, pass_on(UP2, "x", X_NEAR, "z")), (5, pass_on(DOWN2, "y", Y_NEAR, "z")),
                  (5, begin((DOWN2, OWN, "x"), (DOWN2, Y_NEAR, "x"))), (9, pass_on(UP2, "x", DIAG_NEAR))])
    run(pass_on(UP2, "z", X_REST))
    near_core(UP2)
    up(mid, up2_h[0], hid2_h[0], slope2_h[0], [(7, pass_on(UP2, "x", DIAG_REST)), (8, pass_on(DOWN2, "z", Y_REST, "x"))])
    land_all(UP2)
    up(mid, up2_h[1], hid2_h[1], slope2_h[1], [(4, pass_on(DOWN2, "x", X_NEAR, "z"))])
    matmul(hid2, grad, (part_down2,), "tn", (1280, 640), plain, rows_inner=False,
           hooks=[(0, pass_on(DOWN2, "x", DIAG_NEAR)), (1, pass_on(DOWN2, "z", X_REST)), (3, pass_on(DOWN2, "x", DIAG_REST))])
    for m in (DOWN2, DOWN1, UP1):
        land_all(m)
    for part in range(ACT_PARTS):
        act_copy(grad, grad_full, 1, part, "recv")
    assert landed == set(slots)
    for m, piece, way in slots:
        hop(m, piece, way, start=False)
    for part in range(ACT_PARTS):
        act_copy(tok, tok_full, 0, part, "send")
        act_copy(grad, grad_full, 1, part, "send")


def forward(tok, wu1, wd1, wu2, wd2, grad):
    t, h = tok.shape
    r1, c1 = wu1.shape
    r2, c2 = wd1.shape
    ffn = 2 * c1
    shape = jax.ShapeDtypeStruct
    return pl.pallas_call(
        forward_kernel,
        out_shape=(shape((t, 2 * h), BF), shape((t, 2 * h), BF), shape((4 * r1, 2 * c1), BF), shape((4 * r2, 2 * c2), BF),
                   shape((4 * r1, 2 * c1), BF), shape((4 * r2, 2 * c2), BF),
                   shape((t, ffn), BF), shape((t, ffn), F32), shape((t, 2 * h), BF), shape((t, ffn), BF), shape((t, ffn), F32),
                   shape((ffn, h), F32)),
        in_specs=[ANY] * 6,
        out_specs=(ANY,) * 12,
        scratch_shapes=[pltpu.VMEM((2, r1, c1), BF), pltpu.VMEM((2, r2, c2), BF), pltpu.VMEM((2, t, h), BF),
                        pltpu.SemaphoreType.DMA((4, N_SEM)), pltpu.SemaphoreType.DMA((4, N_SEM)),
                        pltpu.SemaphoreType.DMA((2, ACT_PARTS)), pltpu.SemaphoreType.DMA((2, ACT_PARTS)), pltpu.SemaphoreType.DMA((6,))],
        compiler_params=pltpu.CompilerParams(has_side_effects=True, vmem_limit_bytes=60 * 1024 * 1024),
        name="forward",
    )(tok, grad, wu1, wd1, wu2, wd2)


CHUNKS = 8
SLOTS = 4
PERIOD = 8.7


def backward_kernel(*refs):
    (grad, grad_full, tok_full, mid, hid1, hid2, slope1, slope2, up1, down1, up2, down2, part_down2), refs = refs[:13], refs[13:]
    (y_out, grad_x, *outs), refs = refs[:6], refs[6:]
    (dpre2, dmid, dpre1, part_up2, part_down1, part_up1), refs = refs[:6], refs[6:]
    from_twin, from_x, from_in, from_ex = [refs[4 * i:4 * i + 4] for i in range(4)]
    buf_up, buf_down, send, recv, load_sem, store_sem = refs[16:]
    parts = [part_down2, part_up2, part_down1, part_up1]
    here = Place()
    z_end = (here.z == 0) | (here.z == 3)
    inner = jnp.where(here.z == 0, 1, jnp.where(here.z == 3, 2, 3 - here.z))
    outer = jnp.where(here.z < 2, 0, 3)
    total = 4 * CHUNKS
    LOAD, XS, MID, TOT, OUT = 0, 7, 7 + SLOTS, 7 + 2 * SLOTS, 7 + 3 * SLOTS

    def rows_of(i, quarter=None):
        height = parts[i // CHUNKS].shape[0] // 4
        step = height // CHUNKS
        base = (i % CHUNKS) * step
        return pl.ds(base if quarter is None else pl.multiple_of(quarter * height + base, step), step)

    def buf(i, index):
        return (buf_up if parts[i // CHUNKS].shape[1] > 1024 else buf_down).at[index]

    def slot(i, first):
        return buf(i, first + i % SLOTS)

    def part(i, quarter):
        return parts[i // CHUNKS].at[rows_of(i, quarter), :]

    def row_block(ref, i):
        return ref[i // CHUNKS].at[rows_of(i), :]

    def twin(i, which):
        return from_twin[i // CHUNKS].at[which, rows_of(i), :]

    def copy(kind, src, dst, i, device):
        return remote(src, dst, send.at[kind, i], recv.at[kind, i], device)

    def core_copy(i, which):
        x = 1 - here.x if which == 0 else here.x
        return copy(which, part(i, 2 * x + 1 - here.k), twin(i, which), i, here.device(k=1 - here.k))

    def x_copy(i):
        return copy(2, slot(i, XS), row_block(from_x, i), i, here.device(x=1 - here.x))

    def in_copy(i):
        return copy(3, slot(i, MID), row_block(from_in, i), i, here.device(z=inner))

    def ex_copy(i):
        return copy(4, slot(i, TOT), row_block(from_ex, i), i, here.device(z=inner))

    def out_copy(i):
        return copy(5, slot(i, OUT), row_block(outs, i), i, here.device(z=outer))

    def store(i):
        return pltpu.make_async_copy(slot(i, OUT), row_block(outs, i), store_sem.at[i % SLOTS])

    def load(i, index, src):
        return pltpu.make_async_copy(src, buf(i, LOAD + index), load_sem.at[index])

    def add(dst, *srcs):
        height, width = dst.shape
        step = 8 if width > 1024 else 16

        @pl.loop(0, height // step)
        def _(j):
            rows = pl.ds(pl.multiple_of(j * step, step), step)
            value = srcs[0][rows, :]
            for src in srcs[1:]:
                value = value + src[rows, :]
            dst[rows, :] = value

    def start_core(i):
        core_copy(i, 0).start()
        core_copy(i, 1).start()

    def x_loads(i):
        return [load(i, 0, part(i, 2 * (1 - here.x) + here.k)), load(i, 1, twin(i, 0))]

    def mid_loads(i):
        return [load(i, 2, part(i, 2 * here.x + here.k)), load(i, 3, twin(i, 1)), load(i, 4, row_block(from_x, i))]

    def even(j):
        def action():
            cm, ci, ce = j - 2, j - 4, j - 6
            if j + 1 < total:
                start_core(j + 1)
            if j < total:
                for c in x_loads(j):
                    c.wait()
                if j >= SLOTS:
                    x_copy(j - SLOTS).wait_send()
                add(slot(j, XS), buf(j, 0), buf(j, 1))
                x_copy(j).start()
            if 0 <= cm < total:
                for c in mid_loads(cm):
                    c.wait()
                if cm >= SLOTS:
                    @pl.when(z_end)
                    def _():
                        in_copy(cm - SLOTS).wait_send()
                add(slot(cm, MID), buf(cm, 2), buf(cm, 3), buf(cm, 4))

            @pl.when(z_end)
            def _():
                if 0 <= cm < total:
                    in_copy(cm).start()

            @pl.when(~z_end)
            def _():
                if 0 <= ce < total:
                    load(ce, 6, row_block(from_ex, ce)).wait()
                    if ce >= SLOTS:
                        out_copy(ce - SLOTS).wait_send()
                        store(ce - SLOTS).wait()
                    add(slot(ce, OUT), slot(ce, TOT), buf(ce, 6))
                    store(ce).start()
                    out_copy(ce).start()
                if 0 <= ci < total:
                    load(ci, 5, row_block(from_in, ci)).wait()
                    if ci >= SLOTS:
                        ex_copy(ci - SLOTS).wait_send()
                    add(slot(ci, TOT), slot(ci, MID), buf(ci, 5))
                    ex_copy(ci).start()
        return action

    def odd(j):
        def action():
            cx, cm, ci, ce = j + 1, j - 1, j - 3, j - 5
            if cx < total:
                core_copy(cx, 0).wait_recv()
                for c in x_loads(cx):
                    c.start()
            if 0 <= cm < total:
                core_copy(cm, 1).wait_recv()
                x_copy(cm).wait_recv()
                for c in mid_loads(cm):
                    c.start()

            @pl.when(~z_end)
            def _():
                if 0 <= ci < total:
                    in_copy(ci).wait_recv()
                    load(ci, 5, row_block(from_in, ci)).start()
                if 0 <= ce < total:
                    ex_copy(ce).wait_recv()
                    load(ce, 6, row_block(from_ex, ce)).start()
        return action

    actions = [(0.0, 0, odd(-1))]
    for j in range(total + 6):
        actions.append((j * PERIOD + 1.0, min(j + 1, total - 1) // CHUNKS, even(j)))
        actions.append(((j + 0.5) * PERIOD + 1.0, min(j + 1, total - 1) // CHUNKS, odd(j)))

    def my(ref, axis):
        size = ref.shape[axis] // 2
        place = pl.ds(pl.multiple_of(here.y * size, size), size)
        return ref.at[:, place] if axis == 1 else ref.at[place, :]

    def scaled(product, slope):
        return ((product * slope).astype(BF),)

    dpre2_h, slope2_h = halves(dpre2, here.y), halves(slope2, here.y)
    dpre1_h, slope1_h = halves(dpre1, here.y), halves(slope1, here.y)

    def row_halves(ref):
        height = ref.shape[0] // 2
        return [ref.at[pl.ds(pl.multiple_of(h * height, height), height), :] for h in (here.y, 1 - here.y)]

    down2_h, down1_h = row_halves(down2), row_halves(down1)
    dmid_h = halves(dmid, here.y)

    def pre(left, h, down_h, dpre_h, slope_h):
        return lambda hooks: matmul(left, down_h[h], (dpre_h[h],), "nt", (2048, 256), scaled, extra=(slope_h[h],), hooks=hooks)

    def into_mid(hooks):
        matmul(dpre2, up2, (dmid,), "nt", (1024, 256), residual, extra=(grad_full,), rows_inner=False, hooks=hooks)

    tasks = [
        (10, 24, 0, pre(grad_full, 0, down2_h, dpre2_h, slope2_h)),
        (5, 22.5, 1, lambda hooks: matmul(mid, dpre2_h[0], (part_up2,), "tn", (1280, 512), plain, hooks=hooks)),
        (10, 24, 1, pre(grad_full, 1, down2_h, dpre2_h, slope2_h)),
        (10, 37, 1, into_mid),
        (8, 23.5, 2, lambda hooks: matmul(hid1, dmid_h[0], (part_down1,), "tn", (640, 640), plain, rows_inner=False, hooks=hooks)),
        (10, 24, 2, pre(dmid, 0, down1_h, dpre1_h, slope1_h)),
        (5, 22.5, 3, lambda hooks: matmul(tok_full, dpre1_h[0], (part_up1,), "tn", (1280, 512), plain, hooks=hooks)),
        (10, 24, 3, pre(dmid, 1, down1_h, dpre1_h, slope1_h)),
        (8, 24, 3, lambda hooks: matmul(hid2, my(down2, 1), (y_out,), "nn", (256, 640), residual, extra=(my(mid, 1),), hooks=hooks)),
        (8, 24, 3, lambda hooks: matmul(dpre1, my(up1, 0), (grad_x,), "nt", (256, 640), residual, extra=(my(dmid, 1),), hooks=hooks)),
    ]
    start_core(0)
    clock, ready, position = 0.0, 0, 0
    for steps, length, after, call in tasks:
        hooks = []
        for step in range(steps):
            while position < len(actions) and actions[position][0] <= clock and actions[position][1] <= ready:
                hooks.append((step, actions[position][2]))
                position += 1
                clock += 0.6
            clock += length / steps
        call(hooks)
        ready = after
    for _, _, action in actions[position:]:
        action()

    for i in range(total):
        core_copy(i, 0).wait_send()
        core_copy(i, 1).wait_send()
    for i in range(total - SLOTS, total):
        x_copy(i).wait_send()

    @pl.when(z_end)
    def _():
        for i in range(total):
            out_copy(i).wait_recv()
        for i in range(total - SLOTS, total):
            in_copy(i).wait_send()

    @pl.when(~z_end)
    def _():
        for i in range(total - SLOTS, total):
            ex_copy(i).wait_send()
            out_copy(i).wait_send()
            store(i).wait()


def backward(grad, grad_full, tok_full, mid, hid1, hid2, slope1, slope2, up1, down1, up2, down2, part_down2):
    shape = jax.ShapeDtypeStruct
    t, h = grad.shape
    ffn = hid1.shape[1]
    up_part, down_part = (2 * h, ffn // 2), part_down2.shape
    order = [down_part, up_part, down_part, up_part]
    quarters = [(p[0] // 4, p[1]) for p in order]
    outs = [shape((t, h), BF)] * 2 + [shape(q, F32) for q in quarters]
    work = [shape((t, ffn), BF), shape((t, 2 * h), BF), shape((t, ffn), BF), shape(up_part, F32), shape(down_part, F32), shape(up_part, F32)]
    landing = [shape((2,) + q, F32) for q in quarters] + [shape(q, F32) for _ in range(3) for q in quarters]
    n = 4 * CHUNKS
    depth = 7 + 4 * SLOTS
    args = (grad, grad_full, tok_full, mid, hid1, hid2, slope1, slope2, up1, down1, up2, down2, part_down2)
    results = pl.pallas_call(
        backward_kernel,
        out_shape=tuple(outs + work + landing),
        in_specs=[ANY] * len(args),
        out_specs=(ANY,) * (len(outs) + len(work) + len(landing)),
        scratch_shapes=[pltpu.VMEM((depth, quarters[1][0] // CHUNKS, quarters[1][1]), F32), pltpu.VMEM((depth, quarters[0][0] // CHUNKS, quarters[0][1]), F32),
                        pltpu.SemaphoreType.DMA((6, n)), pltpu.SemaphoreType.DMA((6, n)), pltpu.SemaphoreType.DMA((7,)), pltpu.SemaphoreType.DMA((SLOTS,))],
        compiler_params=pltpu.CompilerParams(has_side_effects=True, vmem_limit_bytes=62 * 1024 * 1024),
        name="backward",
    )(*args)
    return results[:6]


def solution(mesh):
    act_spec = P(("dep", "row"), "col")
    weight_spec = P("row", "col")

    def local_step(tokens, w_up1, w_down1, w_up2, w_down2, grad_out):
        (x_full, g_full, up1, down1, up2, down2, hid1, slope1, mid, hid2, slope2, part_down2) = forward(
            tokens, w_up1, w_down1, w_up2, w_down2, grad_out)
        y_out, grad_x, grad_down2, grad_up2, grad_down1, grad_up1 = backward(
            grad_out, g_full, x_full, mid, hid1, hid2, slope1, slope2, up1, down1, up2, down2, part_down2)
        return y_out, grad_x, grad_up1, grad_down1, grad_up2, grad_down2

    return jax.shard_map(local_step, mesh=mesh, in_specs=(act_spec, weight_spec, weight_spec, weight_spec, weight_spec, act_spec), out_specs=(act_spec, act_spec, weight_spec, weight_spec, weight_spec, weight_spec), check_vma=False)
```

```python
import functools

import jax
import jax.numpy as jnp
from jax import lax
from jax.experimental import pallas as pl
from jax.experimental.pallas import tpu as pltpu
from jax.sharding import PartitionSpec as P

BF = jnp.bfloat16
F32 = jnp.float32
ROOT_2_PI = 0.7978845608028654
CUBIC = 0.044715
ANY = pl.BlockSpec(memory_space=pl.ANY)


class Place:
    def __init__(self):
        self.z = lax.axis_index("dep")
        self.y = lax.axis_index("col")
        row = lax.axis_index("row")
        self.x = row // 2
        self.k = row % 2
        self.half = self.z % 2

    def device(self, z=None, y=None, x=None, k=None):
        z = self.z if z is None else z
        y = self.y if y is None else y
        x = self.x if x is None else x
        k = self.k if k is None else k
        return {"dep": z, "col": y, "row": 2 * x + k}


def remote(src, dst, send_sem, recv_sem, device):
    return pltpu.make_async_remote_copy(
        src_ref=src, dst_ref=dst, send_sem=send_sem, recv_sem=recv_sem,
        device_id=device, device_id_type=pl.DeviceIdType.MESH)


def dot(left, right):
    return lax.dot_general(left, right, (((1,), (0,)), ((), ())), preferred_element_type=F32)


def dot_last(left, right):
    return lax.dot_general(left, right, (((1,), (1,)), ((), ())), preferred_element_type=F32)


def dot_first(left, right):
    return lax.dot_general(left, right, (((0,), (0,)), ((), ())), preferred_element_type=F32)


def gelu_pair(pre_act):
    square = pre_act * pre_act
    half = 0.5 + 0.5 * jnp.tanh(pre_act * (ROOT_2_PI + (ROOT_2_PI * CUBIC) * square))
    slope = half + ((half - half * half) * pre_act) * (2 * ROOT_2_PI + (6 * CUBIC * ROOT_2_PI) * square)
    return (pre_act * half).astype(BF), slope


CONTRACT = {"nn": (((1,), (0,)), ((), ())), "nt": (((1,), (1,)), ((), ())), "tn": (((0,), (0,)), ((), ()))}


def matmul(left, right, outs, form, tile, epilogue, extra=(), rows_inner=True, hooks=()):
    depth = left.shape[0] if form == "tn" else left.shape[1]
    rows = left.shape[1] if form == "tn" else left.shape[0]
    cols = right.shape[0] if form == "nt" else right.shape[1]
    tm, tn = tile
    grid = (cols // tn, rows // tm) if rows_inner else (rows // tm, cols // tn)
    assert all(at < grid[0] * grid[1] for at, _ in hooks)

    def spec(shape, index):
        return pl.BlockSpec(shape, (lambda n, m: index(m, n)) if rows_inner else index)

    left_spec = spec((depth, tm), lambda m, n: (0, m)) if form == "tn" else spec((tm, depth), lambda m, n: (m, 0))
    right_spec = spec((tn, depth), lambda m, n: (n, 0)) if form == "nt" else spec((depth, tn), lambda m, n: (0, n))
    tile_spec = spec((tm, tn), lambda m, n: (m, n))

    def body(left_ref, right_ref, *rest):
        step = pl.program_id(0) * grid[1] + pl.program_id(1)
        for at, action in hooks:
            pl.when(step == at)(action)
        product = lax.dot_general(left_ref[...], right_ref[...], CONTRACT[form], preferred_element_type=F32)
        results = epilogue(product, *[ref[...] for ref in rest[:len(extra)]])
        for ref, value in zip(rest[len(extra):], results):
            ref[...] = value

    pltpu.emit_pipeline(body, grid=grid, in_specs=[left_spec, right_spec] + [tile_spec] * len(extra),
                        out_specs=[tile_spec] * len(outs))(left, right, *extra, *outs)


def plain(product):
    return (product,)


def residual(product, base):
    return ((base.astype(F32) + product).astype(BF),)


def halves(ref, y):
    width = ref.shape[1] // 2
    return [ref.at[:, pl.ds(pl.multiple_of(h * width, width), width)] for h in (y, 1 - y)]


def tokens_of(ref, part, parts):
    step = ref.shape[0] // parts
    return ref.at[pl.ds(part * step, step), :]


OWN = (0, 0, 0)
OWN_ALL = (0, 0, 2)
X_NEAR = (1, 0, 0)
X_REST = (1, 0, 1)
X_ALL = (1, 0, 2)
Y_NEAR = (0, 1, 0)
Y_REST = (0, 1, 1)
DIAG_NEAR = (1, 1, 0)
DIAG_REST = (1, 1, 1)
UP1, DOWN1, UP2, DOWN2 = range(4)

N_SEM = 16
ACT_PARTS = 4


def forward_kernel(tok, grad, wu1, wd1, wu2, wd2, tok_full, grad_full, up1, down1, up2, down2,
                   hid1, slope1, mid, hid2, slope2, part_down2,
                   stage_up, stage_down, stage_act, send, recv, act_send, act_recv, local):
    here = Place()

    class Weight:
        def __init__(self, index, own, full):
            self.index, self.own, self.full = index, own, full
            self.rows, self.cols = own.shape

        def slot(self, dx, dy, other, twin=0):
            x = here.x if dx == 0 else 1 - here.x
            y = here.y if dy == 0 else 1 - here.y
            k = here.k if twin == 0 else 1 - here.k
            h = 0 if other == 2 else here.half if other == 0 else 1 - here.half
            height = self.rows if other == 2 else self.rows // 2
            start = pl.multiple_of((2 * x + k) * self.rows + h * height, height)
            return self.full.at[pl.ds(start, height), pl.ds(pl.multiple_of(y * self.cols, self.cols), self.cols)]

        def source(self, piece):
            if piece[:2] != (0, 0):
                return self.slot(*piece)
            if piece[2] == 2:
                return self.own
            h = here.half if piece[2] == 0 else 1 - here.half
            height = self.rows // 2
            return self.own.at[pl.ds(pl.multiple_of(h * height, height), height), :]

    weights = [Weight(i, own, full) for i, (own, full) in enumerate(((wu1, up1), (wd1, down1), (wu2, up2), (wd2, down2)))]
    slots = {}
    landed = set()

    def number(m, piece, way):
        return slots.setdefault((m, piece, way), len([key for key in slots if key[0] == m]))

    def neighbour(way):
        return {"x": here.device(x=1 - here.x), "y": here.device(y=1 - here.y), "z": here.device(z=here.z + 1 - 2 * here.half),
                "core": here.device(k=1 - here.k)}[way]

    def beyond(piece, way):
        dx, dy, other = piece
        return {"x": (1 - dx, dy, other), "y": (dx, 1 - dy, other), "z": (dx, dy, 1 - other if other < 2 else 2), "core": piece}[way]

    def hop(m, piece, way, start=True):
        n = number(m, piece, way)
        copy = remote(weights[m].source(piece), weights[m].slot(*piece), send.at[m, n], recv.at[m, n], neighbour(way))
        if start:
            copy.start()
        else:
            copy.wait_send()

    def land(m, way, piece):
        n = number(m, beyond(piece, way), way)
        landed.add((m, beyond(piece, way), way))
        place = weights[m].slot(*piece, twin=1 if way == "core" else 0)
        remote(place, place, send.at[m, n], recv.at[m, n], neighbour(way)).wait_recv()

    def act_copy(src, full, index, part, wait=None):
        cols, height = src.shape[1], src.shape[0] // ACT_PARTS
        rows = pl.ds(part * height, height)

        def place(y):
            return full.at[rows, pl.ds(pl.multiple_of(y * cols, cols), cols)]

        sems = act_send.at[index, part], act_recv.at[index, part]
        if wait == "recv":
            remote(place(1 - here.y), place(1 - here.y), *sems, neighbour("y")).wait_recv()
            return
        copy = remote(src.at[rows, :], place(here.y), *sems, neighbour("y"))
        if wait == "send":
            copy.wait_send()
        else:
            copy.start()

    def land_all(m):
        for key in [key for key in slots if key[0] == m and key[2] == "core" and key not in landed]:
            land(m, "core", key[1])

    hop(UP1, OWN, "x")
    hop(UP1, OWN, "y")
    hop(UP1, OWN_ALL, "core")
    for part in range(ACT_PARTS):
        if part == ACT_PARTS - 1:
            hop(DOWN1, OWN, "y")
        act_copy(tok, tok_full, 0, part)
    for m in (UP2, DOWN2):
        hop(m, OWN, "y")
    for part in range(ACT_PARTS):
        act_copy(grad, grad_full, 1, part)

    stages = [(wu1, stage_up.at[0], up1), (wd1, stage_down.at[0], down1), (wu2, stage_up.at[1], up2), (wd2, stage_down.at[1], down2)]
    own_places = []
    for src, buf, full in stages:
        rows, cols = src.shape
        own_places.append((src, buf, full.at[pl.ds(pl.multiple_of((2 * here.x + here.k) * rows, rows), rows),
                                             pl.ds(pl.multiple_of(here.y * cols, cols), cols)]))
    for i, (src, full) in enumerate(((tok, tok_full), (grad, grad_full))):
        cols = src.shape[1]
        own_places.append((src, stage_act.at[i], full.at[:, pl.ds(pl.multiple_of(here.y * cols, cols), cols)]))
    for i, (src, buf, place) in enumerate(own_places):
        pltpu.make_async_copy(src, buf, local.at[i]).start()
    outs = []
    for i, (src, buf, place) in enumerate(own_places):
        pltpu.make_async_copy(src, buf, local.at[i]).wait()
        outs.append(pltpu.make_async_copy(buf, place, local.at[i]))
        outs[-1].start()
    for copy in outs:
        copy.wait()

    def pass_on(m, way, piece, *ways):
        def action():
            land(m, way, piece)
            for onward in ways:
                hop(m, piece, onward)
            hop(m, piece, "core")
        return action

    def begin(*sends):
        def action():
            for m, piece, way in sends:
                hop(m, piece, way)
        return action

    def run(*actions):
        for action in actions:
            action()

    def up(act, weight, hid, slope, hooks=()):
        rows = act.shape[0]
        matmul(act, weight, (hid, slope), "nn", (rows, 512 if rows < 2048 else 256), gelu_pair, hooks=hooks)

    up1_h, hid1_h, slope1_h = [halves(ref, here.y) for ref in (up1, hid1, slope1)]

    def up_part(h, first, count, hooks=()):
        height = tok.shape[0] // ACT_PARTS
        rows = pl.ds(first * height, count * height)
        up(tok_full.at[rows, :], up1_h[h], hid1_h[h].at[rows, :], slope1_h[h].at[rows, :], hooks)

    def tokens_land(*parts):
        for part in parts:
            act_copy(tok, tok_full, 0, part, "recv")

    def near_core(m):
        for piece in (OWN_ALL, X_NEAR, X_REST):
            land(m, "core", piece)

    run(pass_on(UP1, "x", X_NEAR, "z"), pass_on(UP1, "y", Y_NEAR, "x", "z"),
        begin((DOWN1, OWN, "x"), (DOWN1, OWN_ALL, "core"), (UP2, OWN_ALL, "core"), (DOWN2, OWN_ALL, "core")),
        pass_on(UP1, "z", X_REST), pass_on(UP1, "x", DIAG_NEAR, "z"))
    near_core(UP1)
    tokens_land(0, 1)
    up_part(0, 0, 2, [(3, pass_on(UP1, "z", Y_REST)), (4, pass_on(DOWN1, "x", X_NEAR))])
    tokens_land(2)
    up_part(0, 2, 1)
    run(pass_on(UP1, "z", DIAG_REST))
    land_all(UP1)
    up_part(1, 0, 2, [(3, pass_on(DOWN1, "y", Y_NEAR, "x", "z")), (3, begin((DOWN1, X_NEAR, "z")))])
    up_part(1, 2, 1)
    run(pass_on(DOWN1, "x", DIAG_NEAR), pass_on(DOWN1, "z", Y_REST, "x"), begin((UP2, OWN, "x")))
    tokens_land(3)
    up_part(0, 3, 1)
    up_part(1, 3, 1, [(2, pass_on(UP2, "y", Y_NEAR, "z", "x"))])
    run(pass_on(DOWN1, "z", X_REST), pass_on(DOWN1, "x", DIAG_REST))
    land_all(DOWN1)
    matmul(hid1, down1, (mid,), "nn", (1024, 256), residual, extra=(tok_full,), rows_inner=False,
           hooks=[(3, pass_on(UP2, "z", Y_REST, "x")), (5, pass_on(UP2, "x", X_NEAR, "z")), (5, pass_on(DOWN2, "y", Y_NEAR, "z")),
                  (5, begin((DOWN2, OWN, "x"), (DOWN2, Y_NEAR, "x"))), (9, pass_on(UP2, "x", DIAG_NEAR))])
    run(pass_on(UP2, "z", X_REST))
    near_core(UP2)
    half_width = up2.shape[1] // 2

    @pl.loop(0, 2)
    def _(turn):
        def rest():
            for piece in (Y_NEAR, Y_REST, DIAG_NEAR, DIAG_REST):
                land(UP2, "core", piece)

        def at_turn(wanted, action):
            def guarded():
                pl.when(turn == wanted)(action)
            return guarded

        pl.when(turn == 1)(rest)
        columns = pl.ds(pl.multiple_of((here.y + turn) % 2 * half_width, half_width), half_width)
        up(mid, up2.at[:, columns], hid2.at[:, columns], slope2.at[:, columns],
           [(7, at_turn(0, pass_on(UP2, "x", DIAG_REST))), (8, at_turn(0, pass_on(DOWN2, "z", Y_REST, "x"))),
            (9, at_turn(1, pass_on(DOWN2, "x", X_NEAR, "z")))])

    matmul(hid2, grad, (part_down2,), "tn", (640, 640), plain, rows_inner=False,
           hooks=[(2, pass_on(DOWN2, "x", DIAG_NEAR)), (6, pass_on(DOWN2, "x", DIAG_REST))])
    run(pass_on(DOWN2, "z", X_REST))
    for m in (DOWN2, DOWN1, UP1):
        land_all(m)
    for part in range(ACT_PARTS):
        act_copy(grad, grad_full, 1, part, "recv")
    assert landed == set(slots)
    for m, piece, way in slots:
        hop(m, piece, way, start=False)
    for part in range(ACT_PARTS):
        act_copy(tok, tok_full, 0, part, "send")
        act_copy(grad, grad_full, 1, part, "send")


def forward(tok, wu1, wd1, wu2, wd2, grad):
    t, h = tok.shape
    r1, c1 = wu1.shape
    r2, c2 = wd1.shape
    ffn = 2 * c1
    shape = jax.ShapeDtypeStruct
    return pl.pallas_call(
        forward_kernel,
        out_shape=(shape((t, 2 * h), BF), shape((t, 2 * h), BF), shape((4 * r1, 2 * c1), BF), shape((4 * r2, 2 * c2), BF),
                   shape((4 * r1, 2 * c1), BF), shape((4 * r2, 2 * c2), BF),
                   shape((t, ffn), BF), shape((t, ffn), F32), shape((t, 2 * h), BF), shape((t, ffn), BF), shape((t, ffn), F32),
                   shape((ffn, h), F32)),
        in_specs=[ANY] * 6,
        out_specs=(ANY,) * 12,
        scratch_shapes=[pltpu.VMEM((2, r1, c1), BF), pltpu.VMEM((2, r2, c2), BF), pltpu.VMEM((2, t, h), BF),
                        pltpu.SemaphoreType.DMA((4, N_SEM)), pltpu.SemaphoreType.DMA((4, N_SEM)),
                        pltpu.SemaphoreType.DMA((2, ACT_PARTS)), pltpu.SemaphoreType.DMA((2, ACT_PARTS)), pltpu.SemaphoreType.DMA((6,))],
        compiler_params=pltpu.CompilerParams(has_side_effects=True, vmem_limit_bytes=60 * 1024 * 1024),
        name="forward",
    )(tok, grad, wu1, wd1, wu2, wd2)


CHUNKS = 8
SLOTS = 4
PERIOD = 8.7


def backward_kernel(*refs):
    (grad, grad_full, tok_full, mid, hid1, hid2, slope1, slope2, up1, down1, up2, down2, part_down2), refs = refs[:13], refs[13:]
    (y_out, grad_x, *outs), refs = refs[:6], refs[6:]
    (dpre2, dmid, dpre1, part_up2, part_down1, part_up1), refs = refs[:6], refs[6:]
    from_twin, from_x, from_in, from_ex = [refs[4 * i:4 * i + 4] for i in range(4)]
    buf_up, buf_down, send, recv, load_sem, store_sem = refs[16:]
    parts = [part_down2, part_up2, part_down1, part_up1]
    here = Place()
    z_end = (here.z == 0) | (here.z == 3)
    inner = jnp.where(here.z == 0, 1, jnp.where(here.z == 3, 2, 3 - here.z))
    outer = jnp.where(here.z < 2, 0, 3)
    total = 4 * CHUNKS
    LOAD, XS, MID, TOT, OUT = 0, 7, 7 + SLOTS, 7 + 2 * SLOTS, 7 + 3 * SLOTS

    def rows_of(i, quarter=None):
        height = parts[i // CHUNKS].shape[0] // 4
        step = height // CHUNKS
        base = (i % CHUNKS) * step
        return pl.ds(base if quarter is None else pl.multiple_of(quarter * height + base, step), step)

    def buf(i, index):
        return (buf_up if parts[i // CHUNKS].shape[1] > 1024 else buf_down).at[index]

    def slot(i, first):
        return buf(i, first + i % SLOTS)

    def part(i, quarter):
        return parts[i // CHUNKS].at[rows_of(i, quarter), :]

    def row_block(ref, i):
        return ref[i // CHUNKS].at[rows_of(i), :]

    def twin(i, which):
        return from_twin[i // CHUNKS].at[which, rows_of(i), :]

    def copy(kind, src, dst, i, device):
        return remote(src, dst, send.at[kind, i], recv.at[kind, i], device)

    def core_copy(i, which):
        x = 1 - here.x if which == 0 else here.x
        return copy(which, part(i, 2 * x + 1 - here.k), twin(i, which), i, here.device(k=1 - here.k))

    def x_copy(i):
        return copy(2, slot(i, XS), row_block(from_x, i), i, here.device(x=1 - here.x))

    def in_copy(i):
        return copy(3, slot(i, MID), row_block(from_in, i), i, here.device(z=inner))

    def ex_copy(i):
        return copy(4, slot(i, TOT), row_block(from_ex, i), i, here.device(z=inner))

    def out_copy(i):
        return copy(5, slot(i, OUT), row_block(outs, i), i, here.device(z=outer))

    def store(i):
        return pltpu.make_async_copy(slot(i, OUT), row_block(outs, i), store_sem.at[i % SLOTS])

    def load(i, index, src):
        return pltpu.make_async_copy(src, buf(i, LOAD + index), load_sem.at[index])

    def add(dst, *srcs):
        height, width = dst.shape
        step = 8 if width > 1024 else 16

        @pl.loop(0, height // step)
        def _(j):
            rows = pl.ds(pl.multiple_of(j * step, step), step)
            value = srcs[0][rows, :]
            for src in srcs[1:]:
                value = value + src[rows, :]
            dst[rows, :] = value

    def start_core(i):
        core_copy(i, 0).start()
        core_copy(i, 1).start()

    def x_loads(i):
        return [load(i, 0, part(i, 2 * (1 - here.x) + here.k)), load(i, 1, twin(i, 0))]

    def mid_loads(i):
        return [load(i, 2, part(i, 2 * here.x + here.k)), load(i, 3, twin(i, 1)), load(i, 4, row_block(from_x, i))]

    def even(j):
        def action():
            cm, ci, ce = j - 2, j - 4, j - 6
            if j + 1 < total:
                start_core(j + 1)
            if j < total:
                for c in x_loads(j):
                    c.wait()
                if j >= SLOTS:
                    x_copy(j - SLOTS).wait_send()
                add(slot(j, XS), buf(j, 0), buf(j, 1))
                x_copy(j).start()
            if 0 <= cm < total:
                for c in mid_loads(cm):
                    c.wait()
                if cm >= SLOTS:
                    @pl.when(z_end)
                    def _():
                        in_copy(cm - SLOTS).wait_send()
                add(slot(cm, MID), buf(cm, 2), buf(cm, 3), buf(cm, 4))

            @pl.when(z_end)
            def _():
                if 0 <= cm < total:
                    in_copy(cm).start()

            @pl.when(~z_end)
            def _():
                if 0 <= ce < total:
                    load(ce, 6, row_block(from_ex, ce)).wait()
                    if ce >= SLOTS:
                        out_copy(ce - SLOTS).wait_send()
                        store(ce - SLOTS).wait()
                    add(slot(ce, OUT), slot(ce, TOT), buf(ce, 6))
                    store(ce).start()
                    out_copy(ce).start()
                if 0 <= ci < total:
                    load(ci, 5, row_block(from_in, ci)).wait()
                    if ci >= SLOTS:
                        ex_copy(ci - SLOTS).wait_send()
                    add(slot(ci, TOT), slot(ci, MID), buf(ci, 5))
                    ex_copy(ci).start()
        return action

    def odd(j):
        def action():
            cx, cm, ci, ce = j + 1, j - 1, j - 3, j - 5
            if cx < total:
                core_copy(cx, 0).wait_recv()
                for c in x_loads(cx):
                    c.start()
            if 0 <= cm < total:
                core_copy(cm, 1).wait_recv()
                x_copy(cm).wait_recv()
                for c in mid_loads(cm):
                    c.start()

            @pl.when(~z_end)
            def _():
                if 0 <= ci < total:
                    in_copy(ci).wait_recv()
                    load(ci, 5, row_block(from_in, ci)).start()
                if 0 <= ce < total:
                    ex_copy(ce).wait_recv()
                    load(ce, 6, row_block(from_ex, ce)).start()
        return action

    actions = [(0.0, 0, odd(-1))]
    for j in range(total + 6):
        actions.append((j * PERIOD + 1.0, min(j + 1, total - 1) // CHUNKS, even(j)))
        actions.append(((j + 0.5) * PERIOD + 1.0, min(j + 1, total - 1) // CHUNKS, odd(j)))

    def my(ref, axis):
        size = ref.shape[axis] // 2
        place = pl.ds(pl.multiple_of(here.y * size, size), size)
        return ref.at[:, place] if axis == 1 else ref.at[place, :]

    def scaled(product, slope):
        return ((product * slope).astype(BF),)

    dpre2_h, slope2_h = halves(dpre2, here.y), halves(slope2, here.y)
    dpre1_h, slope1_h = halves(dpre1, here.y), halves(slope1, here.y)

    def row_halves(ref):
        height = ref.shape[0] // 2
        return [ref.at[pl.ds(pl.multiple_of(h * height, height), height), :] for h in (here.y, 1 - here.y)]

    down2_h, down1_h = row_halves(down2), row_halves(down1)
    dmid_h = halves(dmid, here.y)

    def pre(left, h, down_h, dpre_h, slope_h):
        return lambda hooks: matmul(left, down_h[h], (dpre_h[h],), "nt", (2048, 256), scaled, extra=(slope_h[h],), hooks=hooks)

    def into_mid(hooks):
        matmul(dpre2, up2, (dmid,), "nt", (1024, 256), residual, extra=(grad_full,), rows_inner=False, hooks=hooks)

    tasks = [
        (10, 24, 0, pre(grad_full, 0, down2_h, dpre2_h, slope2_h)),
        (5, 22.5, 1, lambda hooks: matmul(mid, dpre2_h[0], (part_up2,), "tn", (1280, 512), plain, hooks=hooks)),
        (10, 24, 1, pre(grad_full, 1, down2_h, dpre2_h, slope2_h)),
        (10, 37, 1, into_mid),
        (8, 23.5, 2, lambda hooks: matmul(hid1, dmid_h[0], (part_down1,), "tn", (640, 640), plain, rows_inner=False, hooks=hooks)),
        (10, 24, 2, pre(dmid, 0, down1_h, dpre1_h, slope1_h)),
        (5, 22.5, 3, lambda hooks: matmul(tok_full, dpre1_h[0], (part_up1,), "tn", (1280, 512), plain, hooks=hooks)),
        (10, 24, 3, pre(dmid, 1, down1_h, dpre1_h, slope1_h)),
        (8, 24, 3, lambda hooks: matmul(hid2, my(down2, 1), (y_out,), "nn", (256, 640), residual, extra=(my(mid, 1),), hooks=hooks)),
        (8, 24, 3, lambda hooks: matmul(dpre1, my(up1, 0), (grad_x,), "nt", (256, 640), residual, extra=(my(dmid, 1),), hooks=hooks)),
    ]
    start_core(0)
    clock, ready, position = 0.0, 0, 0
    for steps, length, after, call in tasks:
        hooks = []
        for step in range(steps):
            while position < len(actions) and actions[position][0] <= clock and actions[position][1] <= ready:
                hooks.append((step, actions[position][2]))
                position += 1
                clock += 0.6
            clock += length / steps
        call(hooks)
        ready = after
    for _, _, action in actions[position:]:
        action()

    for i in range(total):
        core_copy(i, 0).wait_send()
        core_copy(i, 1).wait_send()
    for i in range(total - SLOTS, total):
        x_copy(i).wait_send()

    @pl.when(z_end)
    def _():
        for i in range(total):
            out_copy(i).wait_recv()
        for i in range(total - SLOTS, total):
            in_copy(i).wait_send()

    @pl.when(~z_end)
    def _():
        for i in range(total - SLOTS, total):
            ex_copy(i).wait_send()
            out_copy(i).wait_send()
            store(i).wait()


def backward(grad, grad_full, tok_full, mid, hid1, hid2, slope1, slope2, up1, down1, up2, down2, part_down2):
    shape = jax.ShapeDtypeStruct
    t, h = grad.shape
    ffn = hid1.shape[1]
    up_part, down_part = (2 * h, ffn // 2), part_down2.shape
    order = [down_part, up_part, down_part, up_part]
    quarters = [(p[0] // 4, p[1]) for p in order]
    outs = [shape((t, h), BF)] * 2 + [shape(q, F32) for q in quarters]
    work = [shape((t, ffn), BF), shape((t, 2 * h), BF), shape((t, ffn), BF), shape(up_part, F32), shape(down_part, F32), shape(up_part, F32)]
    landing = [shape((2,) + q, F32) for q in quarters] + [shape(q, F32) for _ in range(3) for q in quarters]
    n = 4 * CHUNKS
    depth = 7 + 4 * SLOTS
    args = (grad, grad_full, tok_full, mid, hid1, hid2, slope1, slope2, up1, down1, up2, down2, part_down2)
    results = pl.pallas_call(
        backward_kernel,
        out_shape=tuple(outs + work + landing),
        in_specs=[ANY] * len(args),
        out_specs=(ANY,) * (len(outs) + len(work) + len(landing)),
        scratch_shapes=[pltpu.VMEM((depth, quarters[1][0] // CHUNKS, quarters[1][1]), F32), pltpu.VMEM((depth, quarters[0][0] // CHUNKS, quarters[0][1]), F32),
                        pltpu.SemaphoreType.DMA((6, n)), pltpu.SemaphoreType.DMA((6, n)), pltpu.SemaphoreType.DMA((7,)), pltpu.SemaphoreType.DMA((SLOTS,))],
        compiler_params=pltpu.CompilerParams(has_side_effects=True, vmem_limit_bytes=62 * 1024 * 1024),
        name="backward",
    )(*args)
    return results[:6]


def hand_over_kernel(*refs):
    sources, results, buffers = refs[:6], refs[6:12], refs[12:18]
    loads, stores = refs[18:]
    for i, (src, buf) in enumerate(zip(sources, buffers)):
        pltpu.make_async_copy(src, buf, loads.at[i]).start()
    for i, (src, buf, dst) in enumerate(zip(sources, buffers, results)):
        pltpu.make_async_copy(src, buf, loads.at[i]).wait()
        pltpu.make_async_copy(buf, dst, stores.at[i]).start()
    for i, (buf, dst) in enumerate(zip(buffers, results)):
        pltpu.make_async_copy(buf, dst, stores.at[i]).wait()


def hand_over(arrays):
    return pl.pallas_call(
        hand_over_kernel,
        out_shape=tuple(jax.ShapeDtypeStruct(arr.shape, arr.dtype) for arr in arrays),
        in_specs=[ANY] * 6,
        out_specs=(ANY,) * 6,
        scratch_shapes=[pltpu.VMEM(arr.shape, arr.dtype) for arr in arrays] + [pltpu.SemaphoreType.DMA((6,)), pltpu.SemaphoreType.DMA((6,))],
        compiler_params=pltpu.CompilerParams(vmem_limit_bytes=60 * 1024 * 1024),
        name="hand_over",
    )(*arrays)


def solution(mesh):
    act_spec = P(("dep", "row"), "col")
    weight_spec = P("row", "col")

    def local_step(tokens, w_up1, w_down1, w_up2, w_down2, grad_out):
        (x_full, g_full, up1, down1, up2, down2, hid1, slope1, mid, hid2, slope2, part_down2) = forward(
            tokens, w_up1, w_down1, w_up2, w_down2, grad_out)
        y_out, grad_x, grad_down2, grad_up2, grad_down1, grad_up1 = backward(
            grad_out, g_full, x_full, mid, hid1, hid2, slope1, slope2, up1, down1, up2, down2, part_down2)
        return hand_over((y_out, grad_x, grad_up1, grad_down1, grad_up2, grad_down2))

    return jax.shard_map(local_step, mesh=mesh, in_specs=(act_spec, weight_spec, weight_spec, weight_spec, weight_spec, act_spec), out_specs=(act_spec, act_spec, weight_spec, weight_spec, weight_spec, weight_spec), check_vma=False)
```
